512 devices in a mesh: exc: 8 (over z), slab: 64 (over y, x, core).
Axes of the slice: x: 4, y: 8, z: 8, core: 2. Of those that a mesh axis runs over, the one named last changes fastest.
Arguments:
- q_forward: float32 [8, 32768], P('exc', 'slab'), may hold values from -6 to 6
- q_adjoint: float32 [8, 32768], P('exc', 'slab'), may hold values from -6 to 6
- panel_offset: float32 [3, 32768], P(None, 'slab'), may hold values from -0.5 to 0.5
- block_anchor: int32 [3, 256], P(None, 'slab'), may hold values from 0 to 127, as said below
- kernel_hat: float32 [128, 128, 128], P(None, 'slab'), may hold values from 0.05 to 1, as said below
- near_list: int32 [256, 8], P('slab'), may hold values from 0 to 255, as said below
- near_count: int32 [256], P('slab'), may hold values from 1 to 8, as said below
- panel_vertices: int32 [3, 32768], P(None, 'slab'), may hold values from 0 to 16383, as said below
Outputs:
- vertex_grad: float32 [3, 16384], P(None, ('exc', 'slab'))
The draws below stay inside these ranges and needn't reach their ends.
Inputs may be any that keep to these rules, and one draw needn't show every extreme that they name: Block i lies in the planes of slab index i // 4: block_anchor[0, i] // 2 == i // 4. Even in every dimension: kernel_hat[a, b, c] equals kernel_hat[(-a) mod 128, (-b) mod 128, (-c) mod 128]. `near_list`: every entry of a block i's list, valid or not, is a block whose slab index differs from i // 4 by -1, 0 or 1 modulo the number of slab indices. `near_count`: some block has 8 valid entries. `panel_vertices`: vertex v belongs to slab index (v // 32) mod (number of slab indices); the vertices of a panel of block i belong to slab indices that differ from i // 4 by -1, 0 or 1 modulo the number of slab indices.
All inputs are finite; a program needn't handle non-finite values.
Results may differ from the reference program's by a relative error of at most 0.0003.
Values sent between devices are 32-bit elements; how exact they have to be, the bound alone decides.
A program may use at most 192 MiB of HBM per device.

```python
import math
import jax
import jax.numpy as jnp
from jax import lax

G = 128
B = 128
NBD = 4
MAXN = 8
COND = 8
PL = 2
BLOCKS = 256
PANELS = 32768
VCH = 32
V = 16384
N_EXC = 8
N_SLAB = 64


def draw_block_anchor(key, part):
    keys = jax.random.split(jax.random.fold_in(key, 11), 3)
    owner = jnp.arange(BLOCKS, dtype=jnp.int32) // NBD
    plane = owner * PL + jax.random.randint(keys[0], (BLOCKS,), 0, PL, dtype=jnp.int32)
    row = (3 * owner + jax.random.randint(keys[1], (BLOCKS,), -3, 4, dtype=jnp.int32)) % G
    column = (2 * owner + jax.random.randint(keys[2], (BLOCKS,), -3, 4, dtype=jnp.int32)) % G
    return jnp.stack([plane, row, column]).astype(jnp.int32)


def draw_kernel_hat(key, part):
    inner = jax.random.fold_in(key, 13)
    base = jnp.exp(jax.random.uniform(inner, (G, G, G), jnp.float32, math.log(0.05), 0.0))
    mirror = jnp.roll(jnp.flip(base, (0, 1, 2)), 1, (0, 1, 2))
    return 0.5 * (base + mirror)


def draw_near_list(key, part):
    keys = jax.random.split(jax.random.fold_in(key, 17), 2)
    owner = jnp.arange(BLOCKS, dtype=jnp.int32) // NBD
    side = jax.random.randint(keys[0], (BLOCKS, MAXN), -1, 2, dtype=jnp.int32)
    local = jax.random.randint(keys[1], (BLOCKS, MAXN), 0, NBD, dtype=jnp.int32)
    return ((owner[:, None] + side) % N_SLAB * NBD + local).astype(jnp.int32)


def draw_near_count(key, part):
    counts = jax.random.randint(jax.random.fold_in(key, 19), (BLOCKS,), 1, MAXN + 1, dtype=jnp.int32)
    return counts.at[0].set(MAXN)


def draw_panel_vertices(key, part):
    keys = jax.random.split(jax.random.fold_in(key, 23), 3)
    owner = jnp.arange(PANELS, dtype=jnp.int32) // (NBD * B)
    side = jax.random.randint(keys[0], (3, PANELS), -1, 2, dtype=jnp.int32)
    slab_owner = (owner[None, :] + side) % N_SLAB
    part_index = jax.random.randint(keys[1], (3, PANELS), 0, N_EXC, dtype=jnp.int32)
    place = jax.random.randint(keys[2], (3, PANELS), 0, VCH, dtype=jnp.int32)
    return ((part_index * N_SLAB + slab_owner) * VCH + place).astype(jnp.int32)


def block_scale(rng, shape, cuts, least, top_value):
    def one(dim, blocks):
        draws = jax.random.uniform(jax.random.fold_in(jax.random.fold_in(rng, 6), dim), (blocks,), jnp.float32, least / len(cuts), top_value / len(cuts))
        return jnp.repeat(jnp.exp(draws), shape[dim] // blocks).reshape((-1,) + (1,) * (len(shape) - dim - 1))

    level = one(*cuts[0])
    for cut in cuts[1:]:
        level = level * one(*cut)
    return level


def centred(own_key, dims, deviation, most, cuts=(), kind=jnp.bfloat16):
    loudness = block_scale(own_key, dims, cuts, -0.22, 0.18) if cuts else 1.0
    result = jax.random.normal(own_key, dims, jnp.float32) * deviation * loudness
    return jnp.minimum(jnp.maximum(result, -most), most).astype(kind)


def setup_inputs(seed: int = 0) -> dict:
    arg_keys = jax.random.split(jax.random.key(seed), 9)
    return {
        "q_forward": centred(arg_keys[0], (COND, PANELS), 1.0, 6.0, ((0, 8), (1, 64)), jnp.float32),
        "q_adjoint": centred(arg_keys[1], (COND, PANELS), 1.0, 6.0, ((0, 8), (1, 64)), jnp.float32),
        "panel_offset": jnp.clip(jax.random.uniform(arg_keys[2], (3, PANELS), jnp.float32, -0.5, 0.5) * block_scale(arg_keys[2], (3, PANELS), ((1, 64),), -0.4, 0.0), -0.5, 0.5),
        "block_anchor": draw_block_anchor(jax.random.fold_in(arg_keys[8], 71), 0),
        "kernel_hat": draw_kernel_hat(jax.random.fold_in(arg_keys[8], 71), 0),
        "near_list": draw_near_list(jax.random.fold_in(arg_keys[8], 71), 0),
        "near_count": draw_near_count(jax.random.fold_in(arg_keys[8], 71), 0),
        "panel_vertices": draw_panel_vertices(jax.random.fold_in(arg_keys[8], 71), 0),
    }


soften_sq = 16.0
highest = lax.Precision.HIGHEST

def lagrange(offset):
    values = jnp.stack([0.5 * offset * (offset - 1.0), 1.0 - offset * offset, 0.5 * offset * (offset + 1.0)])
    slopes = jnp.stack([offset - 0.5, -2.0 * offset, offset + 0.5])
    return (values, slopes)

def stencil_index(plane, row, column, length, plane_count):
    shifts = jnp.arange(3, dtype=jnp.int32) - 1
    planes = (plane[:, None] + shifts[None, :]) % plane_count
    rows = (row[:, None] + shifts[None, :]) % length
    columns = (column[:, None] + shifts[None, :]) % length
    flat = planes[:, :, None, None] * (length * length) + rows[:, None, :, None] * length + columns[:, None, None, :]
    return flat.reshape(plane.shape[0], 27).astype(jnp.int32)

def block_charges(charges, values):
    return jnp.einsum('fbp,ibp,jbp,kbp->fbijk', charges, values[:, 0], values[:, 1], values[:, 2], precision=highest)

def far_gradient(potential, charges, values, slopes):
    first = jnp.einsum('fbijk,ibp,jbp,kbp->fbp', potential, slopes[:, 0], values[:, 1], values[:, 2], precision=highest)
    second = jnp.einsum('fbijk,ibp,jbp,kbp->fbp', potential, values[:, 0], slopes[:, 1], values[:, 2], precision=highest)
    third = jnp.einsum('fbijk,ibp,jbp,kbp->fbp', potential, values[:, 0], values[:, 1], slopes[:, 2], precision=highest)
    parts = jnp.stack([first, second, third])
    return parts[:, 0] * charges[1][None] + parts[:, 1] * charges[0][None]

def near_gradient(position, forward, adjoint, near_list, near_count):
    mask = (jnp.arange(MAXN, dtype=jnp.int32)[None, :] < near_count[:, None]).astype(jnp.float32)
    groups = BLOCKS // NBD

    def per_group(group):
        rows = (group * NBD + jnp.arange(NBD, dtype=jnp.int32)).astype(jnp.int32)
        own_position = position[:, rows]
        own_forward = forward[:, rows]
        own_adjoint = adjoint[:, rows]
        total = jnp.zeros((3, NBD, B), jnp.float32)
        for slot in range(MAXN):
            other = near_list[rows, slot]
            other_position = position[:, other]
            diff = own_position[:, :, :, None] - other_position[:, :, None, :]
            inverse = lax.rsqrt(lax.optimization_barrier(jnp.sum(diff * diff, axis=0)) + soften_sq)
            pair = jnp.einsum('nbp,nbr->bpr', own_adjoint, forward[:, other], precision=highest)
            pair = pair + jnp.einsum('nbp,nbr->bpr', own_forward, adjoint[:, other], precision=highest)
            weight = pair * inverse * inverse * inverse
            total = total - mask[rows, slot][None, :, None] * lax.optimization_barrier(jnp.sum(diff * weight[None], axis=3))
        return total
    stacked = lax.map(per_group, jnp.arange(groups, dtype=jnp.int32))
    return jnp.transpose(stacked, (1, 0, 2, 3)).reshape(3, BLOCKS, B)

def reference(q_forward, q_adjoint, panel_offset, block_anchor, kernel_hat, near_list, near_count, panel_vertices):
    offset = panel_offset.reshape(3, BLOCKS, B)
    values, slopes = lagrange(offset)
    flat = stencil_index(block_anchor[0], block_anchor[1], block_anchor[2], G, G)
    far_total = jnp.zeros((3, BLOCKS, B), jnp.float32)
    for conductor in range(COND):
        charges = jnp.stack([q_forward[conductor], q_adjoint[conductor]]).reshape(2, BLOCKS, B)
        spread = block_charges(charges, values).reshape(2, -1)
        grid = jnp.zeros((2, G * G * G), jnp.float32).at[:, flat.reshape(-1)].add(spread).reshape(2, G, G, G)
        spectrum = jnp.fft.fftn(grid, axes=(1, 2, 3)) * kernel_hat[None]
        potential = jnp.real(jnp.fft.ifftn(spectrum, axes=(1, 2, 3))).astype(jnp.float32)
        stencil_values = potential.reshape(2, -1)[:, flat].reshape(2, BLOCKS, 3, 3, 3)
        far_total = far_total + far_gradient(stencil_values, charges, values, slopes)
    position = offset + block_anchor.astype(jnp.float32)[:, :, None]
    forward = q_forward.reshape(COND, BLOCKS, B)
    adjoint = q_adjoint.reshape(COND, BLOCKS, B)
    near_total = near_gradient(position, forward, adjoint, near_list, near_count)
    panel_grad = ((far_total + near_total) / (3.0 * COND)).reshape(3, PANELS)
    vertex_grad = jnp.zeros((3, V), jnp.float32)
    for corner in range(3):
        vertex_grad = vertex_grad.at[:, panel_vertices[corner]].add(panel_grad)
    return vertex_grad
```

```python
import functools
import math

import jax
import jax.numpy as jnp
from jax import lax
from jax.experimental import pallas as pl
from jax.experimental.pallas import tpu as pltpu
from jax.sharding import PartitionSpec as P

G = 128
B = 128
VCH = 32
NS = 64
NE = 8
NB = 4
MAXN = 8
MESH = pl.DeviceIdType.MESH
F32 = jnp.float32
BF16 = jnp.bfloat16
soften_sq = 16.0

SIN = [(-1) ** n * (2.0 * math.pi) ** (2 * n + 1) / math.factorial(2 * n + 1) for n in range(7)]


def iota(shape, dim):
    return lax.broadcasted_iota(jnp.int32, shape, dim)


def cos_turns(t):
    w = t - jnp.floor(t + 0.5)
    z = 0.25 - jnp.abs(w)
    z2 = z * z
    p = SIN[6]
    for n in range(5, -1, -1):
        p = SIN[n] + z2 * p
    return z * p


def sin_turns(t):
    return cos_turns(t - 0.25)


def split(a):
    high = a.astype(BF16)
    return high, (a - high.astype(F32)).astype(BF16)


def dot(a, b, nt=False):
    dims = (((1,), (1 if nt else 0,)), ((), ()))
    return lax.dot_general(a, b, dims, preferred_element_type=F32)


def dot3(a, b, nt=False):
    (ah, al), (bh, bl) = a, b
    return dot(ah, bh, nt) + (dot(al, bh, nt) + dot(ah, bl, nt))


def lagrange(t):
    values = [0.5 * t * (t - 1.0), 1.0 - t * t, 0.5 * t * (t + 1.0)]
    slopes = [t - 0.5, -2.0 * t, t + 0.5]
    return values, slopes


def stencil_charges(charges, weights):
    lane = iota((8, 128), 1)
    out = jnp.zeros((8, 128), F32)
    for i in range(3):
        for j in range(3):
            part = charges * weights[0][i] * weights[1][j]
            for k in range(3):
                total = jnp.sum(part * weights[2][k], axis=1, keepdims=True)
                out = jnp.where(lane == 9 * i + 3 * j + k, total, out)
    return out


def lane_tables():
    row = iota((256, 256), 0)
    col = iota((256, 256), 1)
    half = row // 128
    field = (row % 64) // 32
    k = row % 32 % 3 - 1
    part = col // 128
    c = col % 128
    real = jnp.where(half == field, 0.0, jnp.where(half == 0, -0.25, 0.25))
    shift = real + jnp.where(part == 1, 0.25, 0.0)
    return cos_turns((c * k).astype(F32) * (1.0 / G) + shift)


def plane_of(index):
    return jnp.where(index < 64, 2 * index, 2 * index - 127)


def plane_tables():
    r = iota((128, 128), 0)
    c = iota((128, 128), 1)
    forward = (r * plane_of(c)).astype(F32) * (1.0 / G)
    back = (plane_of(r) * c).astype(F32) * (1.0 / G)
    fwd = jnp.concatenate([cos_turns(forward), sin_turns(forward)], axis=1)
    inv = jnp.concatenate([cos_turns(back), sin_turns(back)], axis=1)
    return fwd, inv


def block_phases(x, first_row):
    lane = iota((NS, 128), 1)
    rows = jnp.where(lane < 64, x[:, 28:29], x[:, 92:93])
    j = (lane % 32 // 3 % 3 - 1).astype(F32)
    lanes = []
    for b in range(2):
        t = (rows + j) * ((first_row + b).astype(F32) * (1.0 / G))
        lanes.append((cos_turns(t), sin_turns(t)))
    columns, upper = [], []
    for g in range(2):
        t = x[:, 64 * g + 29 : 64 * g + 30] * (lane.astype(F32) * (1.0 / G))
        columns.append((cos_turns(t), sin_turns(t)))
        upper.append(jnp.broadcast_to(x[:, 64 * g + 27 : 64 * g + 28], (NS, 128)) > 0.5)
    return lanes, columns, upper


def spectrum_to_partials(xs, first_row, table_ref, split_tables, plane_fwd, plane_inv, kernel_rows, roll):
    phases = [block_phases(xs[h], first_row) for h in range(2)]
    rows = []
    for b in range(2):
        for h in range(2):
            cosine, sine = phases[h][0][b]
            rows.append(jnp.concatenate([xs[h] * cosine, xs[h] * sine], axis=1))
    mixed = split(jnp.concatenate(rows, axis=0))
    planes = [[[None, None] for _ in range(4)] for _ in range(2)]

    def add(b, q, part, value):
        old = planes[b][q][part]
        planes[b][q][part] = value if old is None else old + value

    for g in range(2):
        moved = []
        for i in range(3):
            y = dot3(mixed, split_tables(g, i))
            moved.append(y)
        for b in range(2):
            for h in range(2):
                cosine, sine = phases[h][1][g]
                upper = phases[h][2][g]
                at = slice((2 * b + h) * NS, (2 * b + h + 1) * NS)
                v = []
                for i in range(3):
                    yr, yi = moved[i][at, :128], moved[i][at, 128:]
                    v.append((yr * cosine + yi * sine, yi * cosine - yr * sine))
                for part in range(2):
                    low, mid, top = (v[i][part] for i in range(3))
                    add(b, 0, part, jnp.where(upper, 0.0, low))
                    add(b, 1, part, jnp.where(upper, low, mid))
                    add(b, 2, part, jnp.where(upper, mid, top))
                    add(b, 3, part, jnp.where(upper, top, 0.0))
    left, right = [], []
    for b in range(2):
        both = []
        for part in range(2):
            even = planes[b][1][part] + roll(planes[b][3][part], 1, 0)
            odd = planes[b][2][part] + roll(planes[b][0][part], NS - 1, 0)
            both.append(jnp.concatenate([even, odd], axis=0))
        left += both
        right += [both[1], -both[0]]
    stacked = jnp.concatenate(
        [jnp.concatenate(left, axis=1), jnp.concatenate(right, axis=1)], axis=0
    )
    spectrum = dot3(plane_fwd, split(stacked))
    left, right = [], []
    for b in range(2):
        pr = spectrum[:, 256 * b : 256 * b + 128] * kernel_rows[b]
        pi = spectrum[:, 256 * b + 128 : 256 * b + 256] * kernel_rows[b]
        left += [pr, pi]
        right += [-pi, pr]
    stacked = jnp.concatenate(
        [jnp.concatenate(left, axis=1), jnp.concatenate(right, axis=1)], axis=0
    )
    back = dot3(plane_inv, split(stacked))
    levels = []
    for b in range(2):
        parts = []
        for part in range(2):
            at = slice(256 * b + 128 * part, 256 * b + 128 * part + 128)
            even, odd = back[:NS, at], back[NS:, at]
            parts.append([roll(odd, 1, 0), even, odd, roll(even, NS - 1, 0)])
        levels.append(parts)
    total = None
    for g in range(2):
        for i in range(3):
            rows = []
            for b in range(2):
                for h in range(2):
                    cosine, sine = phases[h][1][g]
                    upper = phases[h][2][g]
                    dr, di = (jnp.where(upper, levels[b][part][i + 1], levels[b][part][i]) for part in range(2))
                    rows.append(
                        jnp.concatenate([dr * cosine - di * sine, dr * sine + di * cosine], axis=1)
                    )
            value = dot3(split(jnp.concatenate(rows, axis=0)), split_tables(g, i), nt=True)
            total = value if total is None else total + value
    out = []
    for h in range(2):
        value = None
        for b in range(2):
            cosine, sine = phases[h][0][b]
            at = slice((2 * b + h) * NS, (2 * b + h + 1) * NS)
            part = total[at, :128] * cosine + total[at, 128:] * sine
            value = part if value is None else value + part
        out.append(value)
    return out


def far_rows(potential, weights, slopes):
    first = second = third = None
    for i in range(3):
        plain = turned = leaned = None
        for j in range(3):
            value = slope = None
            for k in range(3):
                at = 9 * i + 3 * j + k
                column = potential[:, at : at + 1]
                a, b = column * weights[2][k], column * slopes[2][k]
                value = a if value is None else value + a
                slope = b if slope is None else slope + b
            a, b, c = value * weights[1][j], value * slopes[1][j], slope * weights[1][j]
            plain = a if plain is None else plain + a
            turned = b if turned is None else turned + b
            leaned = c if leaned is None else leaned + c
        a, b, c = plain * slopes[0][i], turned * weights[0][i], leaned * weights[0][i]
        first = a if first is None else first + a
        second = b if second is None else second + b
        third = c if third is None else third + c
    return first, second, third


def kernel(
    qf_ref,
    qa_ref,
    offset_ref,
    anchor_ref,
    khat_ref,
    near_ref,
    count_ref,
    vertex_ref,
    out_ref,
    charge,
    swapped,
    offs,
    eight,
    message,
    near_send,
    own,
    gathered,
    near_rows,
    khat,
    table_high,
    table_low,
    partial,
    arrived,
    spread,
    near_sum,
    grad,
    owner,
    owed,
    returned,
    local_sem,
    send1,
    recv1,
    near_send_sem,
    near_recv_sem,
    send2,
    recv2,
    send3,
    recv3,
):
    e = lax.axis_index("exc")
    me = lax.axis_index("slab")
    up = lax.rem(me + 1, NS)
    down = lax.rem(me + NS - 1, NS)

    barrier = pltpu.get_barrier_semaphore()

    def greet(k, _):
        pl.semaphore_signal(
            barrier, inc=1, device_id=(e, lax.rem(me + k, NS)), device_id_type=MESH
        )
        return 0

    lax.fori_loop(1, NS, greet, 0)

    def greet_far(k, _):
        other = lax.rem(e + k, NE)
        for at in (down, me, up):
            pl.semaphore_signal(barrier, inc=1, device_id=(other, at), device_id_type=MESH)
        return 0

    lax.fori_loop(1, NE, greet_far, 0)

    kcopy = pltpu.make_async_copy(khat_ref, khat, local_sem)
    kcopy.start()

    for g in range(2):
        for h in range(2):
            m = 2 * g + h
            at = slice(128 * m, 128 * m + 128)
            for f in range(2):
                row = 4 * g + 2 * f + h
                charge[row : row + 1, :] = (qf_ref, qa_ref)[f][0:1, at]
                swapped[row : row + 1, :] = (qa_ref, qf_ref)[f][0:1, at]
                for c in range(3):
                    offs[c, row : row + 1, :] = offset_ref[c : c + 1, at]
            for c in range(3):
                place = offset_ref[c : c + 1, at] + anchor_ref[c, m].astype(F32)
                near_send[4 * c + m : 4 * c + m + 1, :] = place
                own[m, c : c + 1, :] = place
            near_send[12 + m : 13 + m, :] = qf_ref[0:1, at]
            near_send[16 + m : 17 + m, :] = qa_ref[0:1, at]
            own[m, 3:4, :] = qf_ref[0:1, at]
            own[m, 4:5, :] = qa_ref[0:1, at]
    near_send[20:24, :] = jnp.zeros((4, 128), F32)
    near_rows[1, :, :] = near_send[...]
    weights, slopes = [], []
    for c in range(3):
        w, s = lagrange(offs[c])
        weights.append(w)
        slopes.append(s)
    value = stencil_charges(charge[...], weights)
    lane = iota((8, 128), 1)
    row = iota((8, 128), 0)
    for g in range(2):
        for h in range(2):
            m = 2 * g + h
            here = row == 4 * g + h
            plane = (anchor_ref[0, m] - 2 * me).astype(F32)
            for at, number in (
                (27, plane),
                (28, anchor_ref[1, m].astype(F32)),
                (29, anchor_ref[2, m].astype(F32)),
            ):
                value = jnp.where(here & (lane == at), number, value)
    eight[...] = value
    text = eight[0:2, :]
    for t in range(1, 4):
        text = text + pltpu.roll(eight[2 * t : 2 * t + 2, :], 32 * t, 1)
    message[...] = text
    gathered[me] = text

    pl.semaphore_wait(barrier, NS - 1 + 3 * (NE - 1))

    def send_message(k, _):
        pltpu.make_async_remote_copy(
            src_ref=message,
            dst_ref=gathered.at[me],
            send_sem=send1,
            recv_sem=recv1,
            device_id=(e, lax.rem(me + k, NS)),
            device_id_type=MESH,
        ).start()
        return 0

    lax.fori_loop(1, NS, send_message, 0)
    near_up = pltpu.make_async_remote_copy(
        src_ref=near_send,
        dst_ref=near_rows.at[0],
        send_sem=near_send_sem.at[0],
        recv_sem=near_recv_sem.at[0],
        device_id=(e, up),
        device_id_type=MESH,
    )
    near_down = pltpu.make_async_remote_copy(
        src_ref=near_send,
        dst_ref=near_rows.at[2],
        send_sem=near_send_sem.at[1],
        recv_sem=near_recv_sem.at[1],
        device_id=(e, down),
        device_id_type=MESH,
    )
    near_up.start()
    near_down.start()

    base = lane_tables()
    lanes = iota((256, 256), 0) % 128
    for g in range(2):
        for i in range(3):
            mine = (lanes // 64 == g) & (lanes % 32 // 9 == i)
            high, low = split(jnp.where(mine, base, 0.0))
            table_high[3 * g + i] = high
            table_low[3 * g + i] = low
    fwd, inv = plane_tables()
    plane_fwd, plane_inv = split(fwd), split(inv)
    vertex = iota((3 * NE * VCH, 128), 0)
    for m in range(NB):
        hits = None
        for corner in range(3):
            v = vertex_ref[corner : corner + 1, 128 * m : 128 * m + 128]
            span = v // VCH
            relative = (span % NS - me + 1 + NS) % NS
            local = relative * (NE * VCH) + span // NS * VCH + v % VCH
            hit = jnp.where(vertex == local, 1.0, 0.0)
            hits = hit if hits is None else hits + hit
        owner[m] = hits.astype(BF16)

    kcopy.wait()
    kernel_rows = [khat[:, b, :] * (1.0 / (G * G * G)) for b in range(2)]
    pltpu.make_async_copy(gathered.at[pl.ds(0, NS - 1)], gathered.at[pl.ds(0, NS - 1)], recv1).wait()
    xs = [gathered[:, h, :] for h in range(2)]
    parts = spectrum_to_partials(
        xs,
        2 * me,
        None,
        lambda g, i: (table_high[3 * g + i], table_low[3 * g + i]),
        plane_fwd,
        plane_inv,
        kernel_rows,
        pltpu.roll,
    )
    for h in range(2):
        partial[:, h, :] = parts[h]
    arrived[me] = partial[me]

    def send_partial(k, _):
        to = lax.rem(me + k, NS)
        pltpu.make_async_remote_copy(
            src_ref=partial.at[to],
            dst_ref=arrived.at[me],
            send_sem=send2,
            recv_sem=recv2,
            device_id=(e, to),
            device_id_type=MESH,
        ).start()
        return 0

    lax.fori_loop(1, NS, send_partial, 0)

    near_up.wait()
    near_down.wait()
    for side in range(3):
        columns = jnp.transpose(near_rows[side])
        for q in range(5):
            for m in range(NB):
                at = 4 * q + m
                spread[4 * side + m, q] = jnp.broadcast_to(columns[:, at : at + 1], (128, 128))

    def per_block(m, _):
        mine = own[m]
        place = [mine[c : c + 1, :] for c in range(3)]
        forward, adjoint = mine[3:4, :], mine[4:5, :]

        def per_slot(slot, sums):
            other = near_ref[m, slot]
            side = jnp.minimum(lax.rem(other // NB - me + 1 + NS, NS), 2)
            index = side * NB + lax.rem(other, NB)
            keep = jnp.where(slot < count_ref[m], 1.0, 0.0).astype(F32)
            sums = list(sums)
            for chunk in range(4):
                at = pl.ds(32 * chunk, 32)
                diff = [place[c] - spread[index, c, at, :] for c in range(3)]
                square = diff[0] * diff[0] + diff[1] * diff[1] + diff[2] * diff[2]
                inverse = lax.rsqrt(square + soften_sq)
                pair = adjoint * spread[index, 3, at, :] + forward * spread[index, 4, at, :]
                weight = pair * keep * (inverse * inverse * inverse)
                for c in range(3):
                    term = diff[c] * weight
                    sums[c] = sums[c] + (
                        (term[0:8] + term[8:16]) + (term[16:24] + term[24:32])
                    )
            return tuple(sums)

        zero = jnp.zeros((8, 128), F32)
        sums = lax.fori_loop(0, MAXN, per_slot, (zero, zero, zero))
        near_sum[m] = jnp.concatenate(
            [jnp.sum(s, axis=0, keepdims=True) for s in sums] + [jnp.zeros((5, 128), F32)], axis=0
        )
        return 0

    lax.fori_loop(0, NB, per_block, 0)

    pltpu.make_async_copy(arrived.at[pl.ds(0, NS - 1)], arrived.at[pl.ds(0, NS - 1)], recv2).wait()
    potential = jnp.sum(arrived[...], axis=0)
    for t in range(4):
        turned = potential if t == 0 else pltpu.roll(potential, 128 - 32 * t, 1)
        eight[2 * t : 2 * t + 2, :] = turned
    fars = far_rows(eight[...], weights, slopes)
    grad[...] = jnp.zeros((8, NB * B), F32)
    for c in range(3):
        offs[c] = fars[c] * swapped[...]
        for g in range(2):
            for h in range(2):
                m = 2 * g + h
                at = 4 * g + h
                far = offs[c, at : at + 1, :] + offs[c, at + 2 : at + 3, :]
                grad[c : c + 1, 128 * m : 128 * m + 128] = (far - near_sum[m, c : c + 1, :]) * (
                    1.0 / (3.0 * NE)
                )
    total = None
    for m in range(NB):
        whole = grad[:, 128 * m : 128 * m + 128]
        high, rest = split(whole)
        low, last = split(whole - high.astype(F32))
        got = dot(high, owner[m], nt=True) + (dot(low, owner[m], nt=True) + dot(last, owner[m], nt=True))
        total = got if total is None else total + got
    for t in range(6):
        owed[t] = total[0:4, 128 * t : 128 * t + 128]
    returned[3 * e + 1] = owed[2 + e // 4]

    def send_owed(k, _):
        other = lax.rem(e + k, NE)
        for side, at in ((0, down), (1, me), (2, up)):

            def start():
                pltpu.make_async_remote_copy(
                    src_ref=owed.at[2 * side + other // 4],
                    dst_ref=returned.at[3 * e + side],
                    send_sem=send3,
                    recv_sem=recv3,
                    device_id=(other, at),
                    device_id_type=MESH,
                ).start()

            if side == 1:
                pl.when(k > 0)(start)
            else:
                start()
        return 0

    lax.fori_loop(0, NE, send_owed, 0)

    pltpu.make_async_copy(gathered.at[pl.ds(0, NS - 1)], gathered.at[pl.ds(0, NS - 1)], send1).wait()
    pltpu.make_async_copy(partial.at[pl.ds(0, NS - 1)], partial.at[pl.ds(0, NS - 1)], send2).wait()
    count = 3 * NE - 1
    pltpu.make_async_copy(returned.at[pl.ds(0, count)], returned.at[pl.ds(0, count)], recv3).wait()
    result = jnp.sum(returned[...], axis=0)
    pick = lax.rem(e, 4)
    answer = result[0:3, 0:VCH]
    for t in range(1, 4):
        answer = jnp.where(pick == t, pltpu.roll(result, 128 - 32 * t, 1)[0:3, 0:VCH], answer)
    out_ref[...] = answer
    pltpu.make_async_copy(returned.at[pl.ds(0, count)], returned.at[pl.ds(0, count)], send3).wait()


def on_device(qf, qa, offset, anchor, khat, near_list, near_count, vertices):
    vmem = pl.BlockSpec(memory_space=pltpu.VMEM)
    smem = pl.BlockSpec(memory_space=pltpu.SMEM)
    dma = pltpu.SemaphoreType.DMA
    return pl.pallas_call(
        kernel,
        out_shape=jax.ShapeDtypeStruct((3, VCH), F32),
        in_specs=[vmem, vmem, vmem, smem, pl.BlockSpec(memory_space=pl.ANY), smem, smem, vmem],
        out_specs=vmem,
        scratch_shapes=[
            pltpu.VMEM((8, 128), F32),
            pltpu.VMEM((8, 128), F32),
            pltpu.VMEM((3, 8, 128), F32),
            pltpu.VMEM((8, 128), F32),
            pltpu.VMEM((2, 128), F32),
            pltpu.VMEM((24, 128), F32),
            pltpu.VMEM((NB, 8, 128), F32),
            pltpu.VMEM((NS, 2, 128), F32),
            pltpu.VMEM((3, 24, 128), F32),
            pltpu.VMEM((G, 2, G), F32),
            pltpu.VMEM((6, 256, 256), BF16),
            pltpu.VMEM((6, 256, 256), BF16),
            pltpu.VMEM((NS, 2, 128), F32),
            pltpu.VMEM((NS, 2, 128), F32),
            pltpu.VMEM((3 * NB, 5, 128, 128), F32),
            pltpu.VMEM((NB, 8, 128), F32),
            pltpu.VMEM((8, NB * B), F32),
            pltpu.VMEM((NB, 3 * NE * VCH, 128), BF16),
            pltpu.VMEM((6, 4, 128), F32),
            pltpu.VMEM((3 * NE, 4, 128), F32),
            dma(()),
            dma(()),
            dma(()),
            dma((2,)),
            dma((2,)),
            dma(()),
            dma(()),
            dma(()),
            dma(()),
        ],
        compiler_params=pltpu.CompilerParams(collective_id=0, has_side_effects=True),
    )(qf, qa, offset, anchor, khat, near_list, near_count, vertices)


def solution(mesh):
    return jax.shard_map(
        on_device,
        mesh=mesh,
        in_specs=(
            P("exc", "slab"),
            P("exc", "slab"),
            P(None, "slab"),
            P(None, "slab"),
            P(None, "slab", None),
            P("slab", None),
            P("slab"),
            P(None, "slab"),
        ),
        out_specs=P(None, ("exc", "slab")),
        check_vma=False,
    )
```

```python
import functools
import math

import jax
import jax.numpy as jnp
from jax import lax
from jax.experimental import pallas as pl
from jax.experimental.pallas import tpu as pltpu
from jax.sharding import PartitionSpec as P

G = 128
B = 128
VCH = 32
NS = 64
NE = 8
NB = 4
MAXN = 8
MESH = pl.DeviceIdType.MESH
F32 = jnp.float32
BF16 = jnp.bfloat16
soften_sq = 16.0

SIN = [(-1) ** n * (2.0 * math.pi) ** (2 * n + 1) / math.factorial(2 * n + 1) for n in range(7)]


def iota(shape, dim):
    return lax.broadcasted_iota(jnp.int32, shape, dim)


def cos_turns(t):
    w = t - jnp.floor(t + 0.5)
    z = 0.25 - jnp.abs(w)
    z2 = z * z
    p = SIN[6]
    for n in range(5, -1, -1):
        p = SIN[n] + z2 * p
    return z * p


def sin_turns(t):
    return cos_turns(t - 0.25)


def split(a):
    high = a.astype(BF16)
    return high, (a - high.astype(F32)).astype(BF16)


def dot(a, b, nt=False):
    dims = (((1,), (1 if nt else 0,)), ((), ()))
    return lax.dot_general(a, b, dims, preferred_element_type=F32)


def dot3(a, b, nt=False):
    (ah, al), (bh, bl) = a, b
    return dot(ah, bh, nt) + (dot(al, bh, nt) + dot(ah, bl, nt))


def lagrange(t):
    values = [0.5 * t * (t - 1.0), 1.0 - t * t, 0.5 * t * (t + 1.0)]
    slopes = [t - 0.5, -2.0 * t, t + 0.5]
    return values, slopes


def stencil_charges(charges, weights):
    lane = iota((8, 128), 1)
    out = jnp.zeros((8, 128), F32)
    for i in range(3):
        for j in range(3):
            part = charges * weights[0][i] * weights[1][j]
            for k in range(3):
                total = jnp.sum(part * weights[2][k], axis=1, keepdims=True)
                out = jnp.where(lane == 9 * i + 3 * j + k, total, out)
    return out


def lane_tables():
    row = iota((256, 256), 0)
    col = iota((256, 256), 1)
    half = row // 128
    field = (row % 64) // 32
    k = row % 32 % 3 - 1
    part = col // 128
    c = col % 128
    real = jnp.where(half == field, 0.0, jnp.where(half == 0, -0.25, 0.25))
    shift = real + jnp.where(part == 1, 0.25, 0.0)
    return cos_turns((c * k).astype(F32) * (1.0 / G) + shift)


def slab_of(slot):
    return slot % 8 * 8 + slot // 8


def plane_of(index):
    return 2 * slab_of(index % NS) + index // NS


def below(a):
    return jnp.concatenate([pltpu.roll(a[NS - 8 :], 1, 0), a[: NS - 8]], axis=0)


def above(a):
    return jnp.concatenate([a[8:], pltpu.roll(a[:8], 7, 0)], axis=0)


def plane_tables():
    r = iota((128, 128), 0)
    c = iota((128, 128), 1)
    forward = (r * plane_of(c)).astype(F32) * (1.0 / G)
    back = (plane_of(r) * c).astype(F32) * (1.0 / G)
    fwd = jnp.concatenate([cos_turns(forward), sin_turns(forward)], axis=1)
    inv = jnp.concatenate([cos_turns(back), sin_turns(back)], axis=1)
    return fwd, inv


def block_phases(x, first_row):
    lane = iota((NS, 128), 1)
    rows = jnp.where(lane < 64, x[:, 28:29], x[:, 92:93])
    j = (lane % 32 // 3 % 3 - 1).astype(F32)
    lanes = []
    for b in range(2):
        t = (rows + j) * ((first_row + b).astype(F32) * (1.0 / G))
        lanes.append((cos_turns(t), sin_turns(t)))
    columns, upper = [], []
    for g in range(2):
        t = x[:, 64 * g + 29 : 64 * g + 30] * (lane.astype(F32) * (1.0 / G))
        columns.append((cos_turns(t), sin_turns(t)))
        upper.append(jnp.broadcast_to(x[:, 64 * g + 27 : 64 * g + 28], (NS, 128)) > 0.5)
    return lanes, columns, upper


def spectrum_to_partials(xs, first_row, split_tables, plane_fwd, plane_inv, kernel_rows):
    phases = [block_phases(xs[h], first_row) for h in range(2)]
    rows = []
    for b in range(2):
        for h in range(2):
            cosine, sine = phases[h][0][b]
            rows.append(jnp.concatenate([xs[h] * cosine, xs[h] * sine], axis=1))
    mixed = split(jnp.concatenate(rows, axis=0))
    planes = [[[None, None] for _ in range(4)] for _ in range(2)]

    def add(b, q, part, value):
        old = planes[b][q][part]
        planes[b][q][part] = value if old is None else old + value

    for g in range(2):
        moved = []
        for i in range(3):
            y = dot3(mixed, split_tables(g, i))
            moved.append(y)
        for b in range(2):
            for h in range(2):
                cosine, sine = phases[h][1][g]
                upper = phases[h][2][g]
                at = slice((2 * b + h) * NS, (2 * b + h + 1) * NS)
                v = []
                for i in range(3):
                    yr, yi = moved[i][at, :128], moved[i][at, 128:]
                    v.append((yr * cosine + yi * sine, yi * cosine - yr * sine))
                for part in range(2):
                    low, mid, top = (v[i][part] for i in range(3))
                    add(b, 0, part, jnp.where(upper, 0.0, low))
                    add(b, 1, part, jnp.where(upper, low, mid))
                    add(b, 2, part, jnp.where(upper, mid, top))
                    add(b, 3, part, jnp.where(upper, top, 0.0))
    left, right = [], []
    for b in range(2):
        both = []
        for part in range(2):
            even = planes[b][1][part] + below(planes[b][3][part])
            odd = planes[b][2][part] + above(planes[b][0][part])
            both.append(jnp.concatenate([even, odd], axis=0))
        left += both
        right += [both[1], -both[0]]
    stacked = jnp.concatenate(
        [jnp.concatenate(left, axis=1), jnp.concatenate(right, axis=1)], axis=0
    )
    spectrum = dot3(plane_fwd, split(stacked))
    left, right = [], []
    for b in range(2):
        pr = spectrum[:, 256 * b : 256 * b + 128] * kernel_rows[b]
        pi = spectrum[:, 256 * b + 128 : 256 * b + 256] * kernel_rows[b]
        left += [pr, pi]
        right += [-pi, pr]
    stacked = jnp.concatenate(
        [jnp.concatenate(left, axis=1), jnp.concatenate(right, axis=1)], axis=0
    )
    back = dot3(plane_inv, split(stacked))
    levels = []
    for b in range(2):
        parts = []
        for part in range(2):
            at = slice(256 * b + 128 * part, 256 * b + 128 * part + 128)
            even, odd = back[:NS, at], back[NS:, at]
            parts.append([below(odd), even, odd, above(even)])
        levels.append(parts)
    total = None
    for g in range(2):
        for i in range(3):
            rows = []
            for b in range(2):
                for h in range(2):
                    cosine, sine = phases[h][1][g]
                    upper = phases[h][2][g]
                    dr, di = (jnp.where(upper, levels[b][part][i + 1], levels[b][part][i]) for part in range(2))
                    rows.append(
                        jnp.concatenate([dr * cosine - di * sine, dr * sine + di * cosine], axis=1)
                    )
            value = dot3(split(jnp.concatenate(rows, axis=0)), split_tables(g, i), nt=True)
            total = value if total is None else total + value
    out = []
    for h in range(2):
        value = None
        for b in range(2):
            cosine, sine = phases[h][0][b]
            at = slice((2 * b + h) * NS, (2 * b + h + 1) * NS)
            part = total[at, :128] * cosine + total[at, 128:] * sine
            value = part if value is None else value + part
        out.append(value)
    return out


def far_rows(potential, weights, slopes):
    first = second = third = None
    for i in range(3):
        plain = turned = leaned = None
        for j in range(3):
            value = slope = None
            for k in range(3):
                at = 9 * i + 3 * j + k
                column = potential[:, at : at + 1]
                a, b = column * weights[2][k], column * slopes[2][k]
                value = a if value is None else value + a
                slope = b if slope is None else slope + b
            a, b, c = value * weights[1][j], value * slopes[1][j], slope * weights[1][j]
            plain = a if plain is None else plain + a
            turned = b if turned is None else turned + b
            leaned = c if leaned is None else leaned + c
        a, b, c = plain * slopes[0][i], turned * weights[0][i], leaned * weights[0][i]
        first = a if first is None else first + a
        second = b if second is None else second + b
        third = c if third is None else third + c
    return first, second, third


def kernel(
    qf_hbm,
    qa_hbm,
    offset_hbm,
    anchor_hbm,
    khat_hbm,
    near_hbm,
    count_hbm,
    vertex_hbm,
    out_ref,
    qf_ref,
    qa_ref,
    offset_ref,
    anchor_ref,
    near_ref,
    count_ref,
    vertex_ref,
    charge,
    swapped,
    offs,
    eight,
    message,
    near_send,
    own,
    gathered,
    near_rows,
    khat,
    table_high,
    table_low,
    partial,
    arrived,
    spread,
    near_sum,
    grad,
    owner,
    owed,
    returned,
    local_sem,
    send1,
    recv1,
    near_send_sem,
    near_recv_sem,
    send2,
    recv2,
    send3,
    recv3,
):
    e = lax.axis_index("exc")
    me = lax.axis_index("slab")
    up = lax.rem(me + 1, NS)
    down = lax.rem(me + NS - 1, NS)

    wx = lax.rem(me, 8)
    y = me // 8
    slot = 8 * wx + y
    order = (4, 3, 5, 2, 6, 1, 7)
    ys = [lax.rem(y + k, 8) for k in range(8)]
    ws = [lax.rem(wx + k, 8) for k in range(8)]
    steps = [(a, b) for a in range(8) for b in range(8) if a + b > 0]
    steps.sort(key=lambda t: -2 * min(t[0], 8 - t[0]) - min(t[1], 8 - t[1]))
    peers = [(8 * ys[a] + ws[b], 8 * ws[b] + ys[a]) for a, b in steps]

    barrier = pltpu.get_barrier_semaphore()
    for k in order:
        for at in (down, up, me):
            pl.semaphore_signal(
                barrier, inc=1, device_id=(lax.rem(e + k, NE), at), device_id_type=MESH
            )
    for at, _ in peers:
        pl.semaphore_signal(barrier, inc=1, device_id=(e, at), device_id_type=MESH)

    loads = [
        pltpu.make_async_copy(source, target, local_sem.at[n])
        for n, (source, target) in enumerate(
            (
                (qf_hbm, qf_ref),
                (qa_hbm, qa_ref),
                (offset_hbm, offset_ref),
                (anchor_hbm, anchor_ref),
                (khat_hbm, khat),
                (near_hbm, near_ref),
                (count_hbm, count_ref),
                (vertex_hbm, vertex_ref),
            )
        )
    ]
    for load in loads:
        load.start()
    for load in loads[:4]:
        load.wait()

    for g in range(2):
        for h in range(2):
            m = 2 * g + h
            at = slice(128 * m, 128 * m + 128)
            for f in range(2):
                row = 4 * g + 2 * f + h
                charge[row : row + 1, :] = (qf_ref, qa_ref)[f][0:1, at]
                swapped[row : row + 1, :] = (qa_ref, qf_ref)[f][0:1, at]
                for c in range(3):
                    offs[c, row : row + 1, :] = offset_ref[c : c + 1, at]
            for c in range(3):
                place = offset_ref[c : c + 1, at] + anchor_ref[c, m].astype(F32)
                near_send[4 * c + m : 4 * c + m + 1, :] = place
                own[m, c : c + 1, :] = place
            near_send[12 + m : 13 + m, :] = qf_ref[0:1, at]
            near_send[16 + m : 17 + m, :] = qa_ref[0:1, at]
            own[m, 3:4, :] = qf_ref[0:1, at]
            own[m, 4:5, :] = qa_ref[0:1, at]
    near_send[20:24, :] = jnp.zeros((4, 128), F32)
    near_rows[1, :, :] = near_send[...]
    weights, slopes = [], []
    for c in range(3):
        value, slope = lagrange(offs[c])
        weights.append(value)
        slopes.append(slope)
    value = stencil_charges(charge[...], weights)
    lane = iota((8, 128), 1)
    row = iota((8, 128), 0)
    for g in range(2):
        for h in range(2):
            m = 2 * g + h
            here = row == 4 * g + h
            plane = (anchor_ref[0, m] - 2 * me).astype(F32)
            for at, number in (
                (27, plane),
                (28, anchor_ref[1, m].astype(F32)),
                (29, anchor_ref[2, m].astype(F32)),
            ):
                value = jnp.where(here & (lane == at), number, value)
    eight[...] = value
    text = eight[0:2, :]
    for t in range(1, 4):
        text = text + pltpu.roll(eight[2 * t : 2 * t + 2, :], 32 * t, 1)
    message[...] = text
    gathered[slot] = text

    pl.semaphore_wait(barrier, NS - 1 + 3 * (NE - 1))

    for at, _ in peers:
        pltpu.make_async_remote_copy(
            src_ref=message,
            dst_ref=gathered.at[slot],
            send_sem=send1,
            recv_sem=recv1,
            device_id=(e, at),
            device_id_type=MESH,
        ).start()
    near_up = pltpu.make_async_remote_copy(
        src_ref=near_send,
        dst_ref=near_rows.at[0],
        send_sem=near_send_sem.at[0],
        recv_sem=near_recv_sem.at[0],
        device_id=(e, up),
        device_id_type=MESH,
    )
    near_down = pltpu.make_async_remote_copy(
        src_ref=near_send,
        dst_ref=near_rows.at[2],
        send_sem=near_send_sem.at[1],
        recv_sem=near_recv_sem.at[1],
        device_id=(e, down),
        device_id_type=MESH,
    )
    near_up.start()
    near_down.start()

    base = lane_tables()
    lanes = iota((256, 256), 0) % 128
    for g in range(2):
        for i in range(3):
            mine = (lanes // 64 == g) & (lanes % 32 // 9 == i)
            high, low = split(jnp.where(mine, base, 0.0))
            table_high[3 * g + i] = high
            table_low[3 * g + i] = low
    fwd, inv = plane_tables()
    plane_fwd, plane_inv = split(fwd), split(inv)
    loads[7].wait()
    vertex = iota((3 * NE * VCH, 128), 0)
    for m in range(NB):
        hits = None
        for corner in range(3):
            v = vertex_ref[corner : corner + 1, 128 * m : 128 * m + 128]
            span = v // VCH
            relative = (span % NS - me + 1 + NS) % NS
            local = relative * (NE * VCH) + span // NS * VCH + v % VCH
            hit = jnp.where(vertex == local, 1.0, 0.0)
            hits = hit if hits is None else hits + hit
        owner[m] = hits.astype(BF16)

    loads[4].wait()
    kernel_rows = [khat[:, b, :] * (1.0 / (G * G * G)) for b in range(2)]
    most = pl.ds(0, NS - 1)
    pltpu.make_async_copy(gathered.at[most], gathered.at[most], recv1).wait()
    xs = [gathered[:, h, :] for h in range(2)]
    parts = spectrum_to_partials(
        xs,
        2 * me,
        lambda g, i: (table_high[3 * g + i], table_low[3 * g + i]),
        plane_fwd,
        plane_inv,
        kernel_rows,
    )
    for h in range(2):
        partial[:, h, :] = parts[h]
    arrived[slot] = partial[slot]
    for at, theirs in peers:
        pltpu.make_async_remote_copy(
            src_ref=partial.at[theirs],
            dst_ref=arrived.at[slot],
            send_sem=send2,
            recv_sem=recv2,
            device_id=(e, at),
            device_id_type=MESH,
        ).start()

    near_up.wait()
    near_down.wait()
    for side in range(3):
        columns = jnp.transpose(near_rows[side])
        for q in range(5):
            for m in range(NB):
                at = 4 * q + m
                spread[4 * side + m, q] = jnp.broadcast_to(columns[:, at : at + 1], (128, 128))

    loads[5].wait()
    loads[6].wait()

    def per_block(m, _):
        mine = own[m]
        place = [mine[c : c + 1, :] for c in range(3)]
        forward, adjoint = mine[3:4, :], mine[4:5, :]

        def per_slot(slot, sums):
            other = near_ref[m, slot]
            side = jnp.minimum(lax.rem(other // NB - me + 1 + NS, NS), 2)
            index = side * NB + lax.rem(other, NB)
            keep = jnp.where(slot < count_ref[m], 1.0, 0.0).astype(F32)
            sums = list(sums)
            for chunk in range(4):
                at = pl.ds(32 * chunk, 32)
                diff = [place[c] - spread[index, c, at, :] for c in range(3)]
                square = diff[0] * diff[0] + diff[1] * diff[1] + diff[2] * diff[2]
                inverse = lax.rsqrt(square + soften_sq)
                pair = adjoint * spread[index, 3, at, :] + forward * spread[index, 4, at, :]
                weight = pair * keep * (inverse * inverse * inverse)
                for c in range(3):
                    term = diff[c] * weight
                    sums[c] = sums[c] + (
                        (term[0:8] + term[8:16]) + (term[16:24] + term[24:32])
                    )
            return tuple(sums)

        zero = jnp.zeros((8, 128), F32)
        sums = lax.fori_loop(0, MAXN, per_slot, (zero, zero, zero))
        near_sum[m] = jnp.concatenate(
            [jnp.sum(s, axis=0, keepdims=True) for s in sums] + [jnp.zeros((5, 128), F32)], axis=0
        )
        return 0

    lax.fori_loop(0, NB, per_block, 0)

    pltpu.make_async_copy(arrived.at[most], arrived.at[most], recv2).wait()
    potential = jnp.sum(arrived[...], axis=0)
    for t in range(4):
        turned = potential if t == 0 else pltpu.roll(potential, 128 - 32 * t, 1)
        eight[2 * t : 2 * t + 2, :] = turned
    fars = far_rows(eight[...], weights, slopes)
    grad[...] = jnp.zeros((8, NB * B), F32)
    for c in range(3):
        offs[c] = fars[c] * swapped[...]
        for g in range(2):
            for h in range(2):
                m = 2 * g + h
                at = 4 * g + h
                far = offs[c, at : at + 1, :] + offs[c, at + 2 : at + 3, :]
                grad[c : c + 1, 128 * m : 128 * m + 128] = (far - near_sum[m, c : c + 1, :]) * (
                    1.0 / (3.0 * NE)
                )
    total = None
    for m in range(NB):
        whole = grad[:, 128 * m : 128 * m + 128]
        high, rest = split(whole)
        low, last = split(whole - high.astype(F32))
        got = dot(high, owner[m], nt=True) + (dot(low, owner[m], nt=True) + dot(last, owner[m], nt=True))
        total = got if total is None else total + got
    for t in range(6):
        owed[t] = total[0:4, 128 * t : 128 * t + 128]
    returned[3 * e + 1] = owed[2 + e // 4]

    for k in order + (0,):
        other = lax.rem(e + k, NE)
        for side, at in ((0, down), (2, up), (1, me)):
            if k > 0 or side != 1:
                pltpu.make_async_remote_copy(
                    src_ref=owed.at[2 * side + other // 4],
                    dst_ref=returned.at[3 * e + side],
                    send_sem=send3,
                    recv_sem=recv3,
                    device_id=(other, at),
                    device_id_type=MESH,
                ).start()

    pltpu.make_async_copy(gathered.at[most], gathered.at[most], send1).wait()
    pltpu.make_async_copy(partial.at[most], partial.at[most], send2).wait()
    count = 3 * NE - 1
    pltpu.make_async_copy(returned.at[pl.ds(0, count)], returned.at[pl.ds(0, count)], recv3).wait()
    result = jnp.sum(returned[...], axis=0)
    pick = lax.rem(e, 4)
    answer = result[0:3, 0:VCH]
    for t in range(1, 4):
        answer = jnp.where(pick == t, pltpu.roll(result, 128 - 32 * t, 1)[0:3, 0:VCH], answer)
    out_ref[...] = answer
    pltpu.make_async_copy(returned.at[pl.ds(0, count)], returned.at[pl.ds(0, count)], send3).wait()


def on_device(qf, qa, offset, anchor, khat, near_list, near_count, vertices):
    vmem = pl.BlockSpec(memory_space=pltpu.VMEM)
    dma = pltpu.SemaphoreType.DMA
    return pl.pallas_call(
        kernel,
        out_shape=pltpu.VMEM((3, VCH), F32),
        in_specs=[pl.BlockSpec(memory_space=pl.ANY)] * 8,
        out_specs=vmem,
        scratch_shapes=[
            pltpu.VMEM((1, NB * B), F32),
            pltpu.VMEM((1, NB * B), F32),
            pltpu.VMEM((3, NB * B), F32),
            pltpu.SMEM((3, NB), jnp.int32),
            pltpu.SMEM((NB, MAXN), jnp.int32),
            pltpu.SMEM((NB,), jnp.int32),
            pltpu.VMEM((3, NB * B), jnp.int32),
            pltpu.VMEM((8, 128), F32),
            pltpu.VMEM((8, 128), F32),
            pltpu.VMEM((3, 8, 128), F32),
            pltpu.VMEM((8, 128), F32),
            pltpu.VMEM((2, 128), F32),
            pltpu.VMEM((24, 128), F32),
            pltpu.VMEM((NB, 8, 128), F32),
            pltpu.VMEM((NS, 2, 128), F32),
            pltpu.VMEM((3, 24, 128), F32),
            pltpu.VMEM((G, 2, G), F32),
            pltpu.VMEM((6, 256, 256), BF16),
            pltpu.VMEM((6, 256, 256), BF16),
            pltpu.VMEM((NS, 2, 128), F32),
            pltpu.VMEM((NS, 2, 128), F32),
            pltpu.VMEM((3 * NB, 5, 128, 128), F32),
            pltpu.VMEM((NB, 8, 128), F32),
            pltpu.VMEM((8, NB * B), F32),
            pltpu.VMEM((NB, 3 * NE * VCH, 128), BF16),
            pltpu.VMEM((6, 4, 128), F32),
            pltpu.VMEM((3 * NE, 4, 128), F32),
            dma((8,)),
            dma(()),
            dma(()),
            dma((2,)),
            dma((2,)),
            dma(()),
            dma(()),
            dma(()),
            dma(()),
        ],
        compiler_params=pltpu.CompilerParams(collective_id=0, has_side_effects=True),
    )(qf, qa, offset, anchor, khat, near_list, near_count, vertices)


def solution(mesh):
    return jax.shard_map(
        on_device,
        mesh=mesh,
        in_specs=(
            P("exc", "slab"),
            P("exc", "slab"),
            P(None, "slab"),
            P(None, "slab"),
            P(None, "slab", None),
            P("slab", None),
            P("slab"),
            P(None, "slab"),
        ),
        out_specs=P(None, ("exc", "slab")),
        check_vma=False,
    )
```

```python
import jax
import jax.numpy as jnp
from jax import lax
from jax.experimental import pallas as pl
from jax.experimental.pallas import tpu as pltpu
from jax.sharding import PartitionSpec as P

G = 128
B = 128
VCH = 32
NS = 64
NE = 8
NB = 4
MAXN = 8
MESH = pl.DeviceIdType.MESH
F32 = jnp.float32
BF16 = jnp.bfloat16
soften_sq = 16.0

SIN = (6.28318516008872, -41.34165503125344, 81.60100406387009, -76.5497820930982, 39.53670463923752)


def iota(shape, dim):
    return lax.broadcasted_iota(jnp.int32, shape, dim)


def cos_turns(t):
    w = t - jnp.floor(t + 0.5)
    z = 0.25 - jnp.abs(w)
    z2 = z * z
    p = SIN[4]
    for n in range(3, -1, -1):
        p = SIN[n] + z2 * p
    return z * p


def sin_turns(t):
    return cos_turns(t - 0.25)


def split(a):
    high = a.astype(BF16)
    return high, (a - high.astype(F32)).astype(BF16)


def dot(a, b, nt=False):
    dims = (((1,), (1 if nt else 0,)), ((), ()))
    return lax.dot_general(a, b, dims, preferred_element_type=F32)


def dot3(a, b, nt=False):
    (ah, al), (bh, bl) = a, b
    return dot(ah, bh, nt) + (dot(al, bh, nt) + dot(ah, bl, nt))


def lagrange(t):
    values = [0.5 * t * (t - 1.0), 1.0 - t * t, 0.5 * t * (t + 1.0)]
    slopes = [t - 0.5, -2.0 * t, t + 0.5]
    return values, slopes


def stencil_charges(charges, weights):
    lane = iota((8, 128), 1)
    out = jnp.zeros((8, 128), F32)
    for i in range(3):
        for j in range(3):
            part = charges * weights[0][i] * weights[1][j]
            for k in range(3):
                total = jnp.sum(part * weights[2][k], axis=1, keepdims=True)
                out = jnp.where(lane == 9 * i + 3 * j + k, total, out)
    return out


def lane_tables():
    row = iota((256, 256), 0)
    col = iota((256, 256), 1)
    half = row // 128
    field = (row % 64) // 32
    k = row % 32 % 3 - 1
    part = col // 128
    c = col % 128
    real = jnp.where(half == field, 0.0, jnp.where(half == 0, -0.25, 0.25))
    shift = real + jnp.where(part == 1, 0.25, 0.0)
    return cos_turns((c * k).astype(F32) * (1.0 / G) + shift)


def plane_of(row, base):
    return 2 * ((base + row % NS) % NS) + row // NS


def below(a):
    return pltpu.roll(a, 1, 0)


def above(a):
    return pltpu.roll(a, NS - 1, 0)


def plane_tables(base):
    r = iota((128, 128), 0)
    c = iota((128, 128), 1)
    forward = (r * plane_of(c, base)).astype(F32) * (1.0 / G)
    back = (plane_of(r, base) * c).astype(F32) * (1.0 / G)
    fwd = jnp.concatenate([cos_turns(forward), sin_turns(forward)], axis=1)
    inv = jnp.concatenate([cos_turns(back), sin_turns(back)], axis=1)
    return fwd, inv


def block_phases(x, first_row):
    lane = iota((NS, 128), 1)
    rows = jnp.where(lane < 64, x[:, 28:29], x[:, 92:93])
    j = (lane % 32 // 3 % 3 - 1).astype(F32)
    lanes = []
    for b in range(2):
        t = (rows + j) * ((first_row + b).astype(F32) * (1.0 / G))
        lanes.append((cos_turns(t), sin_turns(t)))
    columns, upper = [], []
    for g in range(2):
        t = x[:, 64 * g + 29 : 64 * g + 30] * (lane.astype(F32) * (1.0 / G))
        columns.append((cos_turns(t), sin_turns(t)))
        upper.append(jnp.broadcast_to(x[:, 64 * g + 27 : 64 * g + 28], (NS, 128)))
    return lanes, columns, upper


def spectrum_to_levels(xs, first_row, split_tables, plane_fwd, plane_inv, kernel_rows):
    phases = [block_phases(xs[h], first_row) for h in range(2)]
    rows = []
    for b in range(2):
        for h in range(2):
            cosine, sine = phases[h][0][b]
            rows.append(jnp.concatenate([xs[h] * cosine, xs[h] * sine], axis=1))
    mixed = split(jnp.concatenate(rows, axis=0))
    planes = [[[None, None] for _ in range(4)] for _ in range(2)]

    def add(b, q, part, value):
        old = planes[b][q][part]
        planes[b][q][part] = value if old is None else old + value

    for g in range(2):
        moved = []
        for i in range(3):
            y = dot3(mixed, split_tables(g, i))
            moved.append(y)
        for b in range(2):
            for h in range(2):
                cosine, sine = phases[h][1][g]
                upper = phases[h][2][g] > 0.5
                at = slice((2 * b + h) * NS, (2 * b + h + 1) * NS)
                v = []
                for i in range(3):
                    yr, yi = moved[i][at, :128], moved[i][at, 128:]
                    v.append((yr * cosine + yi * sine, yi * cosine - yr * sine))
                for part in range(2):
                    low, mid, top = (v[i][part] for i in range(3))
                    add(b, 0, part, jnp.where(upper, 0.0, low))
                    add(b, 1, part, jnp.where(upper, low, mid))
                    add(b, 2, part, jnp.where(upper, mid, top))
                    add(b, 3, part, jnp.where(upper, top, 0.0))
    left, right = [], []
    for b in range(2):
        both = []
        for part in range(2):
            even = planes[b][1][part] + below(planes[b][3][part])
            odd = planes[b][2][part] + above(planes[b][0][part])
            both.append(jnp.concatenate([even, odd], axis=0))
        left += both
        right += [both[1], -both[0]]
    stacked = jnp.concatenate(
        [jnp.concatenate(left, axis=1), jnp.concatenate(right, axis=1)], axis=0
    )
    spectrum = dot3(plane_fwd, split(stacked))
    left, right = [], []
    for b in range(2):
        pr = spectrum[:, 256 * b : 256 * b + 128] * kernel_rows[b, :, :]
        pi = spectrum[:, 256 * b + 128 : 256 * b + 256] * kernel_rows[b, :, :]
        left += [pr, pi]
        right += [-pi, pr]
    stacked = jnp.concatenate(
        [jnp.concatenate(left, axis=1), jnp.concatenate(right, axis=1)], axis=0
    )
    back = dot3(plane_inv, split(stacked))
    levels = []
    for b in range(2):
        parts = []
        for part in range(2):
            at = slice(256 * b + 128 * part, 256 * b + 128 * part + 128)
            even, odd = back[:NS, at], back[NS:, at]
            parts.append([below(odd), even, odd, above(even)])
        levels.append(parts)
    return phases, levels


def levels_to_partials(phases, levels, split_tables, pick):
    total = None
    for g in range(2):
        for i in range(3):
            rows = []
            for b in range(2):
                for h in range(2):
                    cosine, sine = (pick(x) for x in phases[h][1][g])
                    upper = pick(phases[h][2][g]) > 0.5
                    dr, di = (
                        jnp.where(upper, pick(levels[b][part][i + 1]), pick(levels[b][part][i]))
                        for part in range(2)
                    )
                    rows.append(
                        jnp.concatenate([dr * cosine - di * sine, dr * sine + di * cosine], axis=1)
                    )
            value = dot3(split(jnp.concatenate(rows, axis=0)), split_tables(g, i), nt=True)
            total = value if total is None else total + value
    size = NS // 2
    out = []
    for h in range(2):
        value = None
        for b in range(2):
            cosine, sine = (pick(x) for x in phases[h][0][b])
            at = slice((2 * b + h) * size, (2 * b + h + 1) * size)
            part = total[at, :128] * cosine + total[at, 128:] * sine
            value = part if value is None else value + part
        out.append(value)
    return out


def far_rows(potential, weights, slopes):
    first = second = third = None
    for i in range(3):
        plain = turned = leaned = None
        for j in range(3):
            value = slope = None
            for k in range(3):
                at = 9 * i + 3 * j + k
                column = potential[:, at : at + 1]
                a, b = column * weights[2][k], column * slopes[2][k]
                value = a if value is None else value + a
                slope = b if slope is None else slope + b
            a, b, c = value * weights[1][j], value * slopes[1][j], slope * weights[1][j]
            plain = a if plain is None else plain + a
            turned = b if turned is None else turned + b
            leaned = c if leaned is None else leaned + c
        a, b, c = plain * slopes[0][i], turned * weights[0][i], leaned * weights[0][i]
        first = a if first is None else first + a
        second = b if second is None else second + b
        third = c if third is None else third + c
    return first, second, third


def kernel(
    qf_hbm,
    qa_hbm,
    offset_hbm,
    anchor_hbm,
    khat_hbm,
    near_hbm,
    count_hbm,
    vertex_hbm,
    out_ref,
    qf_ref,
    qa_ref,
    offset_ref,
    anchor_ref,
    near_ref,
    count_ref,
    vertex_ref,
    charge,
    swapped,
    offs,
    eight,
    message,
    near_send,
    own,
    gathered,
    near_rows,
    khat,
    kernel_rows,
    table_high,
    table_low,
    partial,
    arrived,
    spread,
    near_sum,
    grad,
    owner,
    owed,
    returned,
    local_sem,
    send1,
    recv1,
    near_send_sem,
    near_recv_sem,
    send2,
    recv2,
    send3,
    recv3,
    ready,
):
    e = lax.axis_index("exc")
    me = lax.axis_index("slab")
    up = lax.rem(me + 1, NS)
    down = lax.rem(me + NS - 1, NS)

    wx = lax.rem(me, 8)
    y = me // 8
    order = (4, 3, 5, 2, 6, 1, 7)
    ys = [lax.rem(y + k, 8) for k in range(8)]
    ws = [lax.rem(wx + k, 8) for k in range(8)]
    steps = [(a, b) for a in range(8) for b in range(8) if a + b > 0]
    steps.sort(key=lambda t: -2 * min(t[0], 8 - t[0]) - min(t[1], 8 - t[1]))
    peers = [(8 * ys[a] + ws[b], 8 * a + ws[b], 8 * ((8 - a) % 8) + wx) for a, b in steps]
    far_peers = [p for p, (a, b) in zip(peers, steps) if 2 <= a < 6]
    close_peers = [p for p, (a, b) in zip(peers, steps) if not 2 <= a < 6]

    barrier = pltpu.get_barrier_semaphore()
    for at, _, _ in peers:
        pl.semaphore_signal(barrier, inc=1, device_id=(e, at), device_id_type=MESH)

    for other in range(1, NE):

        @pl.when(other > e)
        def _():
            for at in (down, up, me):
                pl.semaphore_signal(barrier, inc=1, device_id=(other, at), device_id_type=MESH)

    loads = [
        pltpu.make_async_copy(source, target, local_sem.at[n])
        for n, (source, target) in enumerate(
            (
                (qf_hbm, qf_ref),
                (qa_hbm, qa_ref),
                (offset_hbm, offset_ref),
                (anchor_hbm, anchor_ref),
                (khat_hbm, khat),
                (near_hbm, near_ref),
                (count_hbm, count_ref),
                (vertex_hbm, vertex_ref),
            )
        )
    ]
    for load in loads:
        load.start()
    for load in loads[:4]:
        load.wait()

    for g in range(2):
        for h in range(2):
            m = 2 * g + h
            at = slice(128 * m, 128 * m + 128)
            for f in range(2):
                row = 4 * g + 2 * f + h
                charge[row : row + 1, :] = (qf_ref, qa_ref)[f][0:1, at]
                swapped[row : row + 1, :] = (qa_ref, qf_ref)[f][0:1, at]
                for c in range(3):
                    offs[c, row : row + 1, :] = offset_ref[c : c + 1, at]
            for c in range(3):
                place = offset_ref[c : c + 1, at] + anchor_ref[c, m].astype(F32)
                near_send[4 * c + m : 4 * c + m + 1, :] = place
                own[m, c : c + 1, :] = place
            near_send[12 + m : 13 + m, :] = qf_ref[0:1, at]
            near_send[16 + m : 17 + m, :] = qa_ref[0:1, at]
            own[m, 3:4, :] = qf_ref[0:1, at]
            own[m, 4:5, :] = qa_ref[0:1, at]
    near_send[20:24, :] = jnp.zeros((4, 128), F32)
    near_rows[1, :, :] = near_send[...]
    weights, slopes = [], []
    for c in range(3):
        value, slope = lagrange(offs[c])
        weights.append(value)
        slopes.append(slope)
    value = stencil_charges(charge[...], weights)
    lane = iota((8, 128), 1)
    row = iota((8, 128), 0)
    for g in range(2):
        for h in range(2):
            m = 2 * g + h
            here = row == 4 * g + h
            plane = (anchor_ref[0, m] - 2 * me).astype(F32)
            for at, number in (
                (27, plane),
                (28, anchor_ref[1, m].astype(F32)),
                (29, anchor_ref[2, m].astype(F32)),
            ):
                value = jnp.where(here & (lane == at), number, value)
    eight[...] = value
    text = eight[0:2, :]
    for t in range(1, 4):
        text = text + pltpu.roll(eight[2 * t : 2 * t + 2, :], 32 * t, 1)
    message[...] = text
    gathered[wx] = text

    pl.semaphore_wait(barrier, NS - 1 + 3 * e)

    for at, _, there in peers:
        pltpu.make_async_remote_copy(
            src_ref=message,
            dst_ref=gathered.at[there],
            send_sem=send1,
            recv_sem=recv1,
            device_id=(e, at),
            device_id_type=MESH,
        ).start()
    near_up = pltpu.make_async_remote_copy(
        src_ref=near_send,
        dst_ref=near_rows.at[0],
        send_sem=near_send_sem.at[0],
        recv_sem=near_recv_sem.at[0],
        device_id=(e, up),
        device_id_type=MESH,
    )
    near_down = pltpu.make_async_remote_copy(
        src_ref=near_send,
        dst_ref=near_rows.at[2],
        send_sem=near_send_sem.at[1],
        recv_sem=near_recv_sem.at[1],
        device_id=(e, down),
        device_id_type=MESH,
    )
    near_up.start()
    near_down.start()
    for other in range(NE - 1):

        @pl.when(other < e)
        def _():
            for at in (down, up, me):
                pl.semaphore_signal(ready, inc=1, device_id=(other, at), device_id_type=MESH)

    base = lane_tables()
    lanes = iota((256, 256), 0) % 128
    for g in range(2):
        for i in range(3):
            mine = (lanes // 64 == g) & (lanes % 32 // 9 == i)
            high, low = split(jnp.where(mine, base, 0.0))
            table_high[3 * g + i] = high
            table_low[3 * g + i] = low
    fwd, inv = plane_tables(8 * y)
    plane_fwd, plane_inv = split(fwd), split(inv)
    loads[7].wait()
    vertex = iota((3 * NE * VCH, 128), 0)
    for m in range(NB):
        hits = None
        for corner in range(3):
            v = vertex_ref[corner : corner + 1, 128 * m : 128 * m + 128]
            span = v // VCH
            relative = (span % NS - me + 1 + NS) % NS
            local = relative * (NE * VCH) + span // NS * VCH + v % VCH
            hit = jnp.where(vertex == local, 1.0, 0.0)
            hits = hit if hits is None else hits + hit
        owner[m] = hits.astype(BF16)

    loads[4].wait()
    for b in range(2):
        kernel_rows[b] = khat[:, b, :] * (1.0 / (G * G * G))
    most = pl.ds(0, NS - 1)
    pltpu.make_async_copy(gathered.at[most], gathered.at[most], recv1).wait()
    xs = [gathered[:, h, :] for h in range(2)]
    def split_tables(g, i):
        return table_high[3 * g + i], table_low[3 * g + i]

    phases, levels = spectrum_to_levels(
        xs, 2 * me, split_tables, plane_fwd, plane_inv, kernel_rows
    )

    def send_partials(to):
        for at, here, there in to:
            pltpu.make_async_remote_copy(
                src_ref=partial.at[here],
                dst_ref=arrived.at[there],
                send_sem=send2,
                recv_sem=recv2,
                device_id=(e, at),
                device_id_type=MESH,
            ).start()

    parts = levels_to_partials(phases, levels, split_tables, lambda x: x[16:48])
    for h in range(2):
        partial[16:48, h, :] = parts[h]
    send_partials(far_peers)

    @pl.when(me >= 0)
    def _():
        parts = levels_to_partials(
            phases, levels, split_tables, lambda x: jnp.concatenate([x[48:], x[:16]], axis=0)
        )
        for h in range(2):
            partial[48:64, h, :] = parts[h][:16]
            partial[0:16, h, :] = parts[h][16:]

    arrived[wx] = partial[wx]
    send_partials(close_peers)

    near_up.wait()
    near_down.wait()
    for side in range(3):
        columns = jnp.transpose(near_rows[side])
        for q in range(5):
            for m in range(NB):
                at = 4 * q + m
                spread[4 * side + m, q] = jnp.broadcast_to(columns[:, at : at + 1], (128, 128))

    loads[5].wait()
    loads[6].wait()

    def per_block(m, _):
        mine = own[m]
        place = [mine[c : c + 1, :] for c in range(3)]
        forward, adjoint = mine[3:4, :], mine[4:5, :]

        def per_slot(slot, sums):
            other = near_ref[m, slot]
            side = jnp.minimum(lax.rem(other // NB - me + 1 + NS, NS), 2)
            index = side * NB + lax.rem(other, NB)
            keep = jnp.where(slot < count_ref[m], 1.0, 0.0).astype(F32)
            sums = list(sums)
            for chunk in range(4):
                at = pl.ds(32 * chunk, 32)
                diff = [place[c] - spread[index, c, at, :] for c in range(3)]
                square = diff[0] * diff[0] + diff[1] * diff[1] + diff[2] * diff[2]
                inverse = lax.rsqrt(square + soften_sq)
                pair = adjoint * spread[index, 3, at, :] + forward * spread[index, 4, at, :]
                weight = pair * keep * (inverse * inverse * inverse)
                for c in range(3):
                    term = diff[c] * weight
                    sums[c] = sums[c] + (
                        (term[0:8] + term[8:16]) + (term[16:24] + term[24:32])
                    )
            return tuple(sums)

        zero = jnp.zeros((8, 128), F32)
        sums = lax.fori_loop(0, MAXN, per_slot, (zero, zero, zero))
        near_sum[m] = jnp.concatenate(
            [jnp.sum(s, axis=0, keepdims=True) for s in sums] + [jnp.zeros((5, 128), F32)], axis=0
        )
        return 0

    lax.fori_loop(0, NB, per_block, 0)

    pltpu.make_async_copy(arrived.at[most], arrived.at[most], recv2).wait()
    potential = jnp.sum(arrived[...], axis=0)
    for t in range(4):
        turned = potential if t == 0 else pltpu.roll(potential, 128 - 32 * t, 1)
        eight[2 * t : 2 * t + 2, :] = turned
    fars = far_rows(eight[...], weights, slopes)
    grad[...] = jnp.zeros((8, NB * B), F32)
    for c in range(3):
        offs[c] = fars[c] * swapped[...]
        for g in range(2):
            for h in range(2):
                m = 2 * g + h
                at = 4 * g + h
                far = offs[c, at : at + 1, :] + offs[c, at + 2 : at + 3, :]
                grad[c : c + 1, 128 * m : 128 * m + 128] = (far - near_sum[m, c : c + 1, :]) * (
                    1.0 / (3.0 * NE)
                )
    total = None
    for m in range(NB):
        whole = grad[:, 128 * m : 128 * m + 128]
        high, rest = split(whole)
        low, last = split(whole - high.astype(F32))
        got = dot(high, owner[m], nt=True) + (dot(low, owner[m], nt=True) + dot(last, owner[m], nt=True))
        total = got if total is None else total + got
    row = iota((8, 128), 0)
    diagonal = iota((8, 128), 1) // VCH == row
    for t in range(6):
        tile = total[:, 128 * t : 128 * t + 128]
        turns = [tile] + [pltpu.roll(tile, VCH * d, 1) for d in range(1, 4)]
        for part in range(4):
            line = jnp.zeros((8, 128), F32)
            for c in range(3):
                line = jnp.where(diagonal & (row == c), turns[(c - part) % 4], line)
            owed[4 * t + part] = jnp.sum(line, axis=0, keepdims=True)
    returned[3 * e + 1] = owed[NE + e]

    @pl.when(e < NE - 1)
    def _():
        pl.semaphore_wait(ready, 3 * (NE - 1 - e))

    for k in order + (0,):
        other = lax.rem(e + k, NE)
        for side, at in ((0, down), (2, up), (1, me)):
            if k > 0 or side != 1:
                pltpu.make_async_remote_copy(
                    src_ref=owed.at[NE * side + other],
                    dst_ref=returned.at[3 * e + side],
                    send_sem=send3,
                    recv_sem=recv3,
                    device_id=(other, at),
                    device_id_type=MESH,
                ).start()

    pltpu.make_async_copy(gathered.at[most], gathered.at[most], send1).wait()
    pltpu.make_async_copy(partial.at[most], partial.at[most], send2).wait()
    count = 3 * NE - 1
    pltpu.make_async_copy(returned.at[pl.ds(0, count)], returned.at[pl.ds(0, count)], recv3).wait()
    result = jnp.sum(returned[...], axis=0)
    out_ref[0:1, :] = result[:, 0:VCH]
    for c in range(1, 3):
        out_ref[c : c + 1, :] = pltpu.roll(result, 128 - VCH * c, 1)[:, 0:VCH]
    pltpu.make_async_copy(returned.at[pl.ds(0, count)], returned.at[pl.ds(0, count)], send3).wait()


def on_device(qf, qa, offset, anchor, khat, near_list, near_count, vertices):
    vmem = pl.BlockSpec(memory_space=pltpu.VMEM)
    dma = pltpu.SemaphoreType.DMA
    return pl.pallas_call(
        kernel,
        out_shape=pltpu.VMEM((3, VCH), F32),
        in_specs=[pl.BlockSpec(memory_space=pl.ANY)] * 8,
        out_specs=vmem,
        scratch_shapes=[
            pltpu.VMEM((1, NB * B), F32),
            pltpu.VMEM((1, NB * B), F32),
            pltpu.VMEM((3, NB * B), F32),
            pltpu.SMEM((3, NB), jnp.int32),
            pltpu.SMEM((NB, MAXN), jnp.int32),
            pltpu.SMEM((NB,), jnp.int32),
            pltpu.VMEM((3, NB * B), jnp.int32),
            pltpu.VMEM((8, 128), F32),
            pltpu.VMEM((8, 128), F32),
            pltpu.VMEM((3, 8, 128), F32),
            pltpu.VMEM((8, 128), F32),
            pltpu.VMEM((2, 128), F32),
            pltpu.VMEM((24, 128), F32),
            pltpu.VMEM((NB, 8, 128), F32),
            pltpu.VMEM((NS, 2, 128), F32),
            pltpu.VMEM((3, 24, 128), F32),
            pltpu.VMEM((G, 2, G), F32),
            pltpu.VMEM((2, G, G), F32),
            pltpu.VMEM((6, 256, 256), BF16),
            pltpu.VMEM((6, 256, 256), BF16),
            pltpu.VMEM((NS, 2, 128), F32),
            pltpu.VMEM((NS, 2, 128), F32),
            pltpu.VMEM((3 * NB, 5, 128, 128), F32),
            pltpu.VMEM((NB, 8, 128), F32),
            pltpu.VMEM((8, NB * B), F32),
            pltpu.VMEM((NB, 3 * NE * VCH, 128), BF16),
            pltpu.VMEM((3 * NE, 1, 128), F32),
            pltpu.VMEM((3 * NE, 1, 128), F32),
            dma((8,)),
            dma(()),
            dma(()),
            dma((2,)),
            dma((2,)),
            dma(()),
            dma(()),
            dma(()),
            dma(()),
            pltpu.SemaphoreType.REGULAR,
        ],
        compiler_params=pltpu.CompilerParams(collective_id=0, has_side_effects=True),
    )(qf, qa, offset, anchor, khat, near_list, near_count, vertices)


def solution(mesh):
    return jax.shard_map(
        on_device,
        mesh=mesh,
        in_specs=(
            P("exc", "slab"),
            P("exc", "slab"),
            P(None, "slab"),
            P(None, "slab"),
            P(None, "slab", None),
            P("slab", None),
            P("slab"),
            P(None, "slab"),
        ),
        out_specs=P(None, ("exc", "slab")),
        check_vma=False,
    )
```
